32 devices in a mesh: seq: 16 (over z, y, x), ch: 2 (over core).
Axes of the slice: x: 2, y: 2, z: 4, core: 2. Of those that a mesh axis runs over, the one named last changes fastest.
Arguments:
- tokens: bfloat16 [2048, 8192], P('seq', 'ch'), may hold values from -6 to 6
- query_in: bfloat16 [2048, 8192], P('seq', 'ch'), may hold values from -6 to 6
- key_in: bfloat16 [2048, 8192], P('seq', 'ch'), may hold values from -6 to 6
- proj_in: bfloat16 [8192, 1536], P('ch', 'seq'), may hold values from -0.0625 to 0.0625
- proj_out: bfloat16 [1536, 8192], P('seq', 'ch'), may hold values from -0.15625 to 0.15625
- short_taps: float32 [3, 7, 8192], P(None, None, 'ch'), may hold values from -2.4 to 2.4
- residues: float32 [16, 8192], P(None, 'ch'), may hold values from -1.8 to 1.8
- mode_rates: float32 [16, 8192], P(None, 'ch'), may hold values from 0.00024414062 to 0.03
- skip_gain: float32 [8192], P('ch'), may hold values from -3 to 3
Outputs:
- operator_out: bfloat16 [2048, 8192], P('seq', 'ch')
The draws below stay inside these ranges and needn't reach their ends.
All inputs are finite; a program needn't handle non-finite values.
Results may differ from the reference program's by a relative error of at most 0.0069.
Values may be sent and summed in bfloat16 or wider, within the bound.
A program may use at most 192 MiB of HBM per device.

```python
import math
import jax
import jax.numpy as jnp
from jax import lax

D = 8192
R = 1536
SHORT = 7
MODES = 16
SEQ = 2048


def steps_of(key, extent, cuts, low, top_value):
    gain, own = 1.0, jax.random.fold_in(key, 6)
    for axis_at, blocks in cuts:
        draws = jnp.exp(jax.random.uniform(jax.random.fold_in(own, axis_at), (blocks,), jnp.float32, low / len(cuts), top_value / len(cuts)))
        gain = gain * jnp.repeat(draws, extent[axis_at] // blocks).reshape([-1 if axis == axis_at else 1 for axis in range(len(extent))])
    return gain


def bell_draw(stream_key, shape, deviation, most, pieces=(), kind=jnp.bfloat16):
    entries = jax.random.normal(stream_key, shape, jnp.float32) * deviation
    if len(pieces) > 0:
        entries = steps_of(stream_key, shape, pieces, -0.22, 0.18) * entries
    return jnp.clip(entries, min=-most, max=most).astype(kind)


def setup_inputs(seed: int = 0) -> dict:
    key_list = jax.random.split(jax.random.key(seed), 10)
    return {
        "tokens": bell_draw(key_list[0], (SEQ, D), 1.0, 6.0, ((0, 16), (1, 2))),
        "query_in": bell_draw(key_list[1], (SEQ, D), 1.0, 6.0, ((0, 16), (1, 2))),
        "key_in": bell_draw(key_list[2], (SEQ, D), 1.0, 6.0, ((0, 16), (1, 2))),
        "proj_in": bell_draw(key_list[3], (D, R), D ** -0.5, 0.0625, ((0, 2), (1, 16))),
        "proj_out": bell_draw(key_list[4], (R, D), R ** -0.5, 0.15625, ((0, 16), (1, 2))),
        "short_taps": bell_draw(key_list[5], (3, SHORT, D), 0.4, 2.4, ((2, 2),), jnp.float32),
        "residues": bell_draw(key_list[6], (MODES, D), 0.3, 1.8, ((1, 2),), jnp.float32),
        "mode_rates": jnp.clip(jnp.exp(math.log(0.03) - 4.8112082 * jax.random.uniform(key_list[7], (MODES, D), jnp.float32) ** steps_of(key_list[7], (MODES, D), ((1, 2),), -0.2, 0.2)), 0.00024414062, 0.03),
        "skip_gain": bell_draw(key_list[8], (D,), 0.5, 3.0, ((0, 2),), jnp.float32),
    }


def causal_short(signal, filter_taps):
    margin_rows = filter_taps.shape[0] - 1
    length = signal.shape[0]
    padded = jnp.pad(signal, ((margin_rows, 0), (0, 0)))
    result = filter_taps[0] * padded[margin_rows:margin_rows + length]
    for offset in range(1, margin_rows + 1):
        result = result + filter_taps[offset] * padded[margin_rows - offset:margin_rows - offset + length]
    return result

def long_block(operands):
    mixed_block, residue_block, rate_block = operands
    positions = jnp.arange(SEQ).astype(jnp.float32)[:, None]
    impulse = jnp.zeros((SEQ, mixed_block.shape[1]), jnp.float32)
    for mode_index in range(MODES):
        impulse = impulse + residue_block[mode_index] * jnp.sqrt(rate_block[mode_index]) * jnp.exp(-rate_block[mode_index] * positions)
    spectrum = jnp.fft.rfft(mixed_block.astype(jnp.float32), n=2 * SEQ, axis=0) * jnp.fft.rfft(impulse, n=2 * SEQ, axis=0)
    return jnp.fft.irfft(spectrum, n=2 * SEQ, axis=0)[:SEQ].astype(jnp.bfloat16)

def reference(tokens, query_in, key_in, proj_in, proj_out, short_taps, residues, mode_rates, skip_gain):
    low_rank = jnp.dot(tokens, proj_in, preferred_element_type=jnp.float32).astype(jnp.bfloat16)
    value_proj = jnp.dot(low_rank, proj_out, preferred_element_type=jnp.float32).astype(jnp.bfloat16)
    query_short = causal_short(query_in.astype(jnp.float32), short_taps[0])
    key_short = causal_short(key_in.astype(jnp.float32), short_taps[1])
    value_short = causal_short(value_proj.astype(jnp.float32), short_taps[2])
    mixed = (key_short * value_short).astype(jnp.bfloat16)
    blocks = D // 128
    mixed_blocks = mixed.reshape(SEQ, blocks, 128).transpose(1, 0, 2)
    residue_blocks = residues.reshape(MODES, blocks, 128).transpose(1, 0, 2)
    rate_blocks = mode_rates.reshape(MODES, blocks, 128).transpose(1, 0, 2)
    convolved = lax.map(long_block, (mixed_blocks, residue_blocks, rate_blocks))
    convolved = convolved.transpose(1, 0, 2).reshape(SEQ, D)
    return (query_short * (convolved.astype(jnp.float32) + skip_gain * mixed.astype(jnp.float32))).astype(jnp.bfloat16)
```

```python
import functools

import jax
import jax.numpy as jnp
from jax import lax
from jax.experimental import pallas as pl
from jax.experimental.pallas import tpu as pltpu
from jax.sharding import PartitionSpec as P

MESH = pl.DeviceIdType.MESH
VMEM = pl.BlockSpec(memory_space=pltpu.VMEM)
ANY = pl.BlockSpec(memory_space=pl.ANY)
GROUP = 4


def where_am_i():
    me = lax.axis_index("seq")
    return me // GROUP, me % GROUP


def device(plane, spot):
    return {"seq": plane * GROUP + spot}


def remote(source, target, sems, index, place):
    return pltpu.make_async_remote_copy(
        src_ref=source, dst_ref=target, send_sem=sems[0].at[index], recv_sem=sems[1].at[index],
        device_id=place, device_id_type=MESH,
    )


def greet(places):
    barrier = pltpu.get_barrier_semaphore()
    for place in places:
        pl.semaphore_signal(barrier, inc=1, device_id=place, device_id_type=MESH)
    pl.semaphore_wait(barrier, len(places))


def swap(piece, slot, sems, base, plane, spot):
    copies = []
    for step in range(1, GROUP):
        peer = (spot + step) % GROUP
        copies.append(remote(piece(peer), slot(spot), sems, base + step - 1, device(plane, peer)))
    return copies


def multiple(value, by):
    return pl.multiple_of(value, by)


class Place:
    def __init__(self):
        self.me, self.core = lax.axis_index("seq"), lax.axis_index("ch")
        self.count = lax.axis_size("seq")
        self.plane, self.spot = self.me // GROUP, self.me % GROUP
        plane, spot = self.plane, self.spot
        self.side = plane // 2
        self.outer = (self.side + plane + 1) % 2
        self.mate, self.cross = plane + 1 - 2 * (plane % 2), 3 - plane
        self.far = 3 - self.mate
        self.peers = [spot, spot + 1 - 2 * (spot % 2), (spot + 2) % GROUP, 3 - spot]
        self.partner = {"ch": 1 - self.core}

    def at_outer(self, run):
        pl.when(self.outer == 1)(run)

    def at_inner(self, run):
        pl.when(self.outer == 0)(run)


CUTS = 4
AGAIN = range(1, GROUP)
W1A, W2A, TOK, KEY = 0, 3, 6, 9
W1M, W1C, TOKM = 12, 16, 24
W2M, W2C, W2CM, W2O, W2F = 28, 32, 36, 40, 44
PAIR, RS, LZ, AG, LD = 48, 52, 64, 66, 72
EDGE, QT, KT = 80, 81, 82
COPIES = 83


def fetch_all(
    tok, pin, pout, key, query, low_out, rows_out, key_all, query_edge,
    w1, tok_all, w2, key_more, partial, inbox, summed, parts, mylow, lowout, low_all,
    send, recv, local,
):
    p = Place()
    plane, spot, core, peers = p.plane, p.spot, p.core, p.peers
    rows, ranks, width = tok.shape[0], pin.shape[0], w2.shape[-1]
    margin, half = query_edge.shape[0], rows // 2
    share, both = GROUP * ranks, GROUP * GROUP * ranks
    wide, sub = both // 2, width // CUTS
    after = {"seq": (p.me + 1) % p.count}
    before = {"seq": (p.me + p.count - 1) % p.count}

    barrier = pltpu.get_barrier_semaphore()
    greeted = [device(plane, peers[k]) for k in AGAIN]
    greeted += [device(p.mate, spot), p.partner, after, before]
    for place in greeted:
        pl.semaphore_signal(barrier, inc=1, device_id=place, device_id_type=MESH)

    @p.at_inner
    def _():
        pl.semaphore_signal(barrier, inc=1, device_id=device(p.cross, spot), device_id_type=MESH)

    pl.semaphore_wait(barrier, len(greeted) + 1 - p.outer)

    def go(source, target, index, place):
        return remote(source, target, (send, recv), index, place)

    def cols(s):
        return pl.ds(multiple(s * width, width), width)

    def w1_rows(at, s):
        return pl.ds(multiple((at * GROUP + s) * ranks, ranks), ranks)

    def tok_rows(b, s):
        return pl.ds(multiple((b * GROUP + s) * rows, rows), rows)

    def cut(c):
        return slice(c * sub, (c + 1) * sub)

    def halves(h):
        return pl.ds(multiple(h * wide, wide), wide)

    def low_rows(s, j):
        return pl.ds(multiple(margin + s * rows + j * half, margin), half)

    def scatter(source, target, base):
        return [go(source(peers[k]), target, base + k - 1, device(plane, peers[k])) for k in AGAIN]

    mate_dev, cross_dev = device(p.mate, spot), device(p.cross, spot)
    mine1 = w1.at[w1_rows(plane, spot)]
    w1_swap = scatter(lambda s: pin.at[:, cols(s)], mine1, W1A)
    tok_swap = scatter(lambda s: tok.at[:, cols(s)], tok_all.at[tok_rows(p.outer, spot)], TOK)
    w2_swap = scatter(lambda s: pout.at[:, cols(s)], w2.at[plane, spot], W2A)
    key_swap = scatter(lambda s: key_more.at[:, cols(s)], key_all.at[spot], KEY)
    tails = [
        go(key.at[pl.ds(rows - margin, margin)], key_more.at[pl.ds(0, margin)], KT, after),
        go(query.at[pl.ds(rows - margin, margin)], query_edge, QT, after),
    ]

    def own_or(first, arrived, k):
        return first if k == 0 else arrived

    w1_mate = [
        go(own_or(pin.at[:, cols(spot)], w1.at[w1_rows(plane, peers[k])], k),
           w1.at[w1_rows(plane, peers[k])], W1M + k, mate_dev) for k in range(GROUP)]
    w1_cross = [
        go(own_or(pin.at[:, cols(spot)], w1.at[w1_rows(plane, peers[k])], k),
           w1.at[w1_rows(plane, peers[k])], W1C + k, cross_dev) for k in range(GROUP)]
    w1_on = [
        go(w1.at[w1_rows(p.mate, peers[k])], w1.at[w1_rows(p.mate, peers[k])],
           W1C + GROUP + k, cross_dev) for k in range(GROUP)]
    tok_mate = [
        go(own_or(tok.at[:, cols(spot)], tok_all.at[tok_rows(1, peers[k])], k),
           tok_all.at[tok_rows(1, peers[k])], TOKM + k, mate_dev) for k in range(GROUP)]

    def strip(at, c, base, place):
        block = w2.at[at, :, :, cut(c)]
        return go(block, block, base + c, place)

    every = range(CUTS)
    w2_mate = [strip(plane, c, W2M, mate_dev) for c in every]
    w2_cross = [strip(plane, c, W2C, cross_dev) for c in every]
    w2_on = [strip(p.mate, c, W2CM, cross_dev) for c in every]
    w2_out = [strip(p.cross, c, W2O, mate_dev) for c in every]
    w2_far = [strip(p.far, c, W2F, mate_dev) for c in every]

    def low_piece(h):
        return mylow.at[:, halves(h)]

    sides = [p.side, 1 - p.side]

    def run(copies, what):
        for copy in copies:
            getattr(copy, what)()

    run(w1_swap, "start")
    p.at_outer(w1_mate[0].start)
    p.at_inner(w1_cross[0].start)
    run(tails, "start")
    run(w2_swap, "start")
    run(tok_swap, "start")
    w1[w1_rows(plane, spot), :] = pin[:, cols(spot)]
    tok_all[tok_rows(p.outer, spot), :] = tok[:, cols(spot)]
    keep = [
        pltpu.make_async_copy(pout.at[:, cols(spot)], w2.at[plane, spot], local.at[0]),
        pltpu.make_async_copy(key, key_more.at[pl.ds(margin, rows)], local.at[1]),
    ]
    run(keep, "start")
    run(keep, "wait")
    last = pltpu.make_async_copy(key_more.at[:, cols(spot)], key_all.at[spot], local.at[2])

    def unit(b, h):
        for n in range(wide // 256):
            place = pl.ds(multiple(sides[h] * wide + n * 256, 256), 256)
            found = lax.dot_general(
                tok_all[b * GROUP * rows:(b + 1) * GROUP * rows, :], w1[place, :],
                (((1,), (1,)), ((), ())), preferred_element_type=jnp.float32)
            partial[b, :, :, :, place] = found.reshape(GROUP, 2, half, 256)

    def pair(b, h):
        return go(partial.at[b, :, 1 - core, :, halves(sides[h])],
                  inbox.at[b, :, :, halves(sides[h])], PAIR + 2 * b + h, p.partner)

    def reduced(b, h):
        return [
            go(summed.at[b, peers[k], :, halves(sides[h])],
               parts.at[k - 1, b, :, halves(sides[h])], RS + 6 * b + 3 * h + k - 1,
               device(plane, peers[k])) for k in AGAIN]

    def add_pair(b, h):
        pair(b, h).wait_recv()
        place = halves(sides[h])
        for s in range(GROUP):
            summed[b, s, :, place] = (
                partial[b, s, core, :, place] + inbox[b, s, :, place]).astype(summed.dtype)
        run(reduced(b, h), "start")

    def finish(b, h):
        run(reduced(b, h), "wait_recv")
        place = halves(sides[h])
        total = partial[b, spot, core, :, place] + inbox[b, spot, :, place]
        for k in AGAIN:
            total = total + parts[k - 1, b, :, place].astype(jnp.float32)
        target = lowout if b else mylow
        target[:, place] = total.astype(target.dtype)

    def low_up(h):
        return go(lowout.at[:, halves(h)], mylow.at[:, halves(h)], LZ + h, mate_dev)

    def gather(h):
        return [
            go(mylow.at[:, halves(h)], low_all.at[low_rows(spot, core), halves(h)],
               AG + 3 * h + k - 1, device(plane, peers[k])) for k in AGAIN]

    def across(h, k):
        block = low_all.at[low_rows(peers[k], core), halves(h)]
        return go(own_or(mylow.at[:, halves(h)], block, k), block, LD + 4 * h + k, p.partner)

    def spread_low(h):
        run(gather(h), "start")
        across(h, 0).start()
        low_all[low_rows(spot, core), halves(h)] = mylow[:, halves(h)]

    @p.at_outer
    def _():
        for k in (1, 2, 3):
            w1_swap[k - 1].wait_recv()
            w1_mate[k].start()
        tok_mate[0].start()
        run(tails, "wait_recv")
        run(key_swap, "start")
        last.start()
        for k in (1, 2, 3):
            tok_swap[k - 1].wait_recv()
            tok_mate[k].start()
        run(w2_swap, "wait_recv")
        run(w2_mate, "start")

    @p.at_inner
    def _():
        def forward(copies, on, which):
            for k in which:
                copies[k].wait_recv()
                on[k].start()

        for k in (1, 2):
            w1_swap[k - 1].wait_recv()
            w1_cross[k].start()
        forward(w1_mate, w1_on, (0,))
        w1_swap[2].wait_recv()
        w1_cross[3].start()
        forward(w1_mate, w1_on, (1, 2, 3))
        run(w2_swap, "wait_recv")
        run(w2_mate, "start")
        run(w2_cross, "start")
        run(tok_swap, "wait_recv")
        unit(0, 0)
        pair(0, 0).start()
        run(tails, "wait_recv")
        add_pair(0, 0)
        run(key_swap, "start")
        last.start()
        run(w1_cross + w1_on, "wait_recv")
        unit(0, 1)
        pair(0, 1).start()
        add_pair(0, 1)
        forward(w2_cross, w2_out, (0,))
        run(tok_mate, "wait_recv")
        unit(1, 0)
        pair(1, 0).start()
        unit(1, 1)
        pair(1, 1).start()
        add_pair(1, 0)
        forward(w2_cross, w2_out, (1,))
        add_pair(1, 1)
        finish(0, 0)
        finish(0, 1)
        for h in range(2):
            spread_low(sides[h])
        forward(w2_mate, w2_on, (0,))
        finish(1, 0)
        low_up(sides[0]).start()
        forward(w2_cross, w2_out, (2,))
        finish(1, 1)
        low_up(sides[1]).start()
        forward(w2_mate, w2_on, (1,))
        forward(w2_cross, w2_out, (3,))
        forward(w2_mate, w2_on, (2, 3))

    @p.at_outer
    def _():
        for h in (0, 1):
            low_up(sides[1 - h]).wait_recv()
            spread_low(sides[1 - h])

    for h in (0, 1):
        for k in AGAIN:
            gather(h)[k - 1].wait_recv()
            across(h, k).start()

    @p.at_inner
    def _():
        for c in every:
            w2_on[c].wait_recv()
            w2_far[c].start()

    for h in (0, 1):
        for k in range(GROUP):
            across(h, k).wait_recv()
    above = go(low_all.at[pl.ds(low_all.shape[0] - margin, margin)],
               low_all.at[pl.ds(0, margin)], EDGE, device((plane + 1) % GROUP, spot))
    pl.when(plane < GROUP - 1)(above.start)

    @p.at_outer
    def _():
        run(w2_mate + w2_out + w2_far, "wait_recv")

    pl.when(plane > 0)(above.wait_recv)

    @pl.when(plane == 0)
    def _():
        low_all[0:margin, :] = jnp.zeros((margin, both), low_all.dtype)

    out = [
        pltpu.make_async_copy(low_all, low_out, local.at[3]),
        pltpu.make_async_copy(w2, rows_out, local.at[4]),
    ]
    run(out, "start")
    run(key_swap, "wait_recv")
    last.wait()
    run(w1_swap + w2_swap + tok_swap + key_swap + tails, "wait_send")
    for h in (0, 1):
        run(gather(h) + [across(h, k) for k in range(GROUP)], "wait_send")
    pl.when(plane < GROUP - 1)(above.wait_send)
    run(w2_mate, "wait_send")

    @p.at_outer
    def _():
        run(w1_mate + tok_mate, "wait_send")

    @p.at_inner
    def _():
        run(w1_cross + w1_on + w2_cross + w2_on + w2_out + w2_far, "wait_send")
        for b in range(2):
            for h in range(2):
                pair(b, h).wait_send()
                run(reduced(b, h), "wait_send")
        for h in range(2):
            low_up(h).wait_send()

    run(out, "wait")


def share_states(mine, ends, send, recv, local):
    plane, spot = where_am_i()
    peers = [device((plane + step) % GROUP, spot) for step in range(1, GROUP)]
    greet(peers)
    copies = [
        remote(mine, ends.at[plane], (send, recv), index, peer) for index, peer in enumerate(peers)
    ]
    for copy in copies:
        copy.start()
    keep = pltpu.make_async_copy(mine, ends.at[plane], local.at[0])
    keep.start()
    for copy in copies:
        copy.wait()
    keep.wait()


def give_back(mine, out, send, recv, local):
    plane, spot = where_am_i()
    rows, width = out.shape[0], mine.shape[1]
    greet([device(plane, (spot + step) % GROUP) for step in range(1, GROUP)])

    def piece(peer):
        return mine.at[pl.ds(pl.multiple_of(peer * rows, rows), rows)]

    def slot(s):
        return out.at[:, pl.ds(pl.multiple_of(s * width, width), width)]

    moved = swap(piece, slot, (send, recv), 0, plane, spot)
    for copy in moved:
        copy.start()
    keep = pltpu.make_async_copy(piece(spot), slot(spot), local.at[0])
    keep.start()
    for copy in moved:
        copy.wait_recv()
    for copy in moved:
        copy.wait_send()
    keep.wait()


def talk(kernel, shapes, in_specs, scratch, copies, locals_, ident):
    one = not isinstance(shapes, (list, tuple))
    return pl.pallas_call(
        kernel,
        out_shape=shapes,
        in_specs=in_specs,
        out_specs=ANY if one else [ANY] * len(shapes),
        scratch_shapes=scratch + [
            pltpu.SemaphoreType.DMA((copies,)),
            pltpu.SemaphoreType.DMA((copies,)),
            pltpu.SemaphoreType.DMA((locals_,)),
        ],
        compiler_params=pltpu.CompilerParams(collective_id=ident, has_side_effects=True),
    )


def tile_of(source, row, target, place):
    tall, lanes = target.shape[-2:]
    start = where_am_i()[1] * (tall * lanes)
    for column in range(tall):
        cols = pl.ds(pl.multiple_of(start + column * lanes, lanes), lanes)
        target[(*place, pl.ds(column, 1))] = source[(*row, cols)]


def end_states(
    value, key, all_taps, all_rates, spread, states, values, keys, taps, decay
):
    modes, tall, lanes = decay.shape
    for mode in range(modes):
        tile_of(all_rates, (pl.ds(mode, 1),), decay, (mode,))
        decay[mode] = jnp.exp(-decay[mode])
    for branch in range(2):
        for tap in range(taps.shape[1]):
            tile_of(all_taps, (branch + 1, pl.ds(tap, 1)), taps, (branch, tap))
    margin = value.shape[0] - spread.shape[0] // tall
    count, rows = taps.shape[1], spread.shape[0] // tall
    piece = key.shape[1] - margin

    def lay(target, start, load):
        for column in range(tall):
            tile = load(slice(column * lanes, (column + 1) * lanes)).astype(jnp.float32)
            target[pl.ds(start * tall + column, 16, stride=tall), :] = tile

    @pl.loop(0, value.shape[0] // 16)
    def _(block):
        start = pl.multiple_of(block * 16, 16)
        lay(values, start, lambda cols: value[pl.ds(start, 16), cols])

    for edge in range(0, margin, 16):
        lay(keys, edge, lambda cols: key[0, edge:edge + 16, cols])
    for part in range(key.shape[0]):

        @pl.loop(0, piece // 16)
        def _(block):
            start = pl.multiple_of(block * 16, 16)
            lay(keys, margin + part * piece + start,
                lambda cols: key[part, pl.ds(margin + start, 16), cols])

    on = (where_am_i()[0] > 0).astype(jnp.float32)
    for row in range(margin):
        for target in (values, keys):
            place = slice(row * tall, (row + 1) * tall)
            target[place, :] = target[place, :] * on

    rates = [decay[mode] for mode in range(modes)]
    gains = [[taps[branch, tap] for tap in range(count)] for branch in range(2)]

    def short(source, gain, at):
        total = None
        for tap in range(count):
            place = pl.ds(pl.multiple_of((at + margin - tap) * tall, tall), tall)
            term = gain[tap] * source[place, :]
            total = term if total is None else total + term
        return total

    def step(at, held):
        for part in range(4):
            now = at * 4 + part
            mixed = short(keys, gains[0], now) * short(values, gains[1], now)
            mixed = mixed.astype(jnp.bfloat16).astype(jnp.float32)
            spread[pl.ds(pl.multiple_of(now * tall, tall), tall), :] = mixed
            held = [h * r + mixed for h, r in zip(held, rates)]
        return held

    held = lax.fori_loop(0, rows // 4, step, [jnp.zeros((tall, lanes), jnp.float32)] * modes)
    for mode in range(modes):
        states[mode] = held[mode]


def run_states(spread, ends, all_rates, residues, skip, out, kept, rate, weight, gains):
    modes, tall, lanes = rate.shape
    rows = out.shape[0]
    plane = where_am_i()[0]
    for mode in range(modes):
        tile_of(all_rates, (pl.ds(mode, 1),), rate, (mode,))
        tile_of(residues, (pl.ds(mode, 1),), weight, (mode,))
    tile_of(skip, (pl.ds(0, 1),), gains, ())
    rates = [jnp.exp(-rate[mode]) for mode in range(modes)]
    weights = [weight[mode] * jnp.sqrt(rate[mode]) for mode in range(modes)]
    gain = gains[...]

    def step(at, held):
        for part in range(4):
            place = pl.ds(pl.multiple_of((at * 4 + part) * tall, tall), tall)
            value = spread[place, :]
            held = [h * r + value for h, r in zip(held, rates)]
            terms = [h * w for h, w in zip(held, weights)]
            while len(terms) > 1:
                terms = [a + b for a, b in zip(terms[::2], terms[1::2])]
            rounded = terms[0].astype(jnp.bfloat16).astype(jnp.float32)
            kept[place, :] = rounded + gain * value
        return held

    carried = []
    for mode in range(modes):
        total = jnp.zeros((tall, lanes), jnp.float32)
        for at in range(ends.shape[0] - 1):
            longer = total * jnp.exp(-rate[mode] * rows) + ends[at, mode]
            total = jnp.where(at < plane, longer, total)
        carried.append(total)
    lax.fori_loop(0, rows // 4, step, carried)

    @pl.loop(0, rows // 16)
    def _(block):
        start = pl.multiple_of(block * 16, 16)
        for column in range(tall):
            tile = kept[pl.ds(start * tall + column, 16, stride=tall), :]
            out[pl.ds(start, 16), column * lanes:(column + 1) * lanes] = tile.astype(jnp.bfloat16)


def planes_device(
    tokens, query_in, key_in, proj_in, proj_out, short_taps, residues, mode_rates, skip_gain
):
    rows, channels = tokens.shape
    ranks = proj_in.shape[1]
    modes = residues.shape[0]
    margin_rows = short_taps.shape[1] - 1
    width, all_rows = channels // GROUP, rows * GROUP
    tall = width // 128
    half = jnp.bfloat16
    shape = jax.ShapeDtypeStruct
    plane, spot = where_am_i()
    margin = 16
    share, both = GROUP * ranks, GROUP * GROUP * ranks

    full, band = jnp.float32, rows // 2
    low_all, rows_all, key_all, query_edge = talk(
        fetch_all,
        [shape((margin + all_rows, both), half), shape((GROUP, GROUP, ranks, width), half),
         shape((GROUP, margin + rows, width), half), shape((margin, channels), half)],
        [VMEM] * 5,
        [pltpu.VMEM((both, width), half), pltpu.VMEM((2 * all_rows, width), half),
         pltpu.VMEM((GROUP, GROUP, ranks, width), half), pltpu.VMEM((margin + rows, channels), half),
         pltpu.VMEM((2, GROUP, 2, band, both), full), pltpu.VMEM((2, GROUP, band, both), full),
         pltpu.VMEM((2, GROUP, band, both), half), pltpu.VMEM((GROUP - 1, 2, band, both), half),
         pltpu.VMEM((band, both), half), pltpu.VMEM((band, both), half),
         pltpu.VMEM((margin + all_rows, both), half)],
        COPIES, 7, 5,
    )(tokens, proj_in.T, proj_out, key_in, query_in)
    value = jnp.dot(
        low_all, rows_all.reshape(both, width), preferred_element_type=jnp.float32).astype(half)

    tiles, tile = (modes, tall, 128), (tall, 128)
    scattered = pltpu.VMEM(((margin + all_rows) * tall, 128), jnp.float32)
    spread, states = pl.pallas_call(
        end_states,
        out_shape=[shape((all_rows * tall, 128), jnp.float32), shape(tiles, jnp.float32)],
        in_specs=[VMEM] * 4, out_specs=[VMEM] * 2,
        scratch_shapes=[
            scattered, scattered, pltpu.VMEM((2, margin_rows + 1, *tile), jnp.float32),
            pltpu.VMEM(tiles, jnp.float32)],
    )(value, key_all, short_taps, mode_rates)
    ends = talk(share_states, shape((GROUP, *tiles), jnp.float32), [VMEM], [], 3, 1, 2)(states)
    mixed_out = pl.pallas_call(
        run_states,
        out_shape=shape((all_rows, width), half),
        in_specs=[VMEM] * 5, out_specs=VMEM,
        scratch_shapes=[
            pltpu.VMEM((all_rows * tall, 128), jnp.float32), pltpu.VMEM(tiles, jnp.float32),
            pltpu.VMEM(tiles, jnp.float32), pltpu.VMEM(tile, jnp.float32)],
    )(spread, ends, mode_rates, residues, skip_gain[None])
    given = talk(give_back, shape((rows, channels), half), [VMEM], [], 3, 1, 3)(mixed_out)
    first = lax.axis_index("seq") == 0
    query_previous = jnp.where(first, 0, query_edge[margin - margin_rows:]).astype(half)
    query_short = short_filter(query_previous, query_in, short_taps[0])
    return (query_short * given.astype(jnp.float32)).astype(half)


precise = lax.Precision.HIGHEST


def carried_in(value, axis, join, neutral):
    count, mine = (lax.axis_size(axis), lax.axis_index(axis))
    pieces = jax.tree.map(lambda part: lax.all_gather(part, axis), value)
    total = jax.tree.map(
        lambda part, zero: jnp.full_like(part, 0) + jnp.asarray(zero, part.dtype), value, neutral
    )

    def turn(position, total):
        longer = join(total, jax.tree.map(lambda part: part[position], pieces))
        return jax.tree.map(lambda new, old: jnp.where(position < mine, new, old), longer, total)

    return lax.fori_loop(0, count - 1, turn, total)


def passed_along(value, axis, steps):
    count = lax.axis_size(axis)
    leading, last = (max(0, -steps), min(count, count - steps))
    return lax.ppermute(value, axis, [(source, source + steps) for source in range(leading, last)])


def short_filter(previous, current, filter_taps):
    margin_rows = filter_taps.shape[0] - 1
    length = current.shape[0]
    extended = jnp.concatenate([previous, current], axis=0).astype(jnp.float32)
    result = filter_taps[0] * extended[margin_rows : margin_rows + length]
    for offset in range(1, margin_rows + 1):
        result = (
            result
            + filter_taps[offset] * extended[margin_rows - offset : margin_rows - offset + length]
        )
    return result


def carry_states(earlier, later):
    return (earlier[0] * later[1] + later[0], earlier[1] * later[1])


def modal_convolve(mixed, residues, mode_rates):
    tok_rows = mixed.shape[0]
    signal = mixed.astype(jnp.float32)
    steps = jnp.arange(tok_rows, dtype=jnp.int32)
    lower = (steps[:, None] >= steps[None, :]).astype(jnp.float32)
    centred = (steps.astype(jnp.float32) - 0.5 * tok_rows)[:, None]
    local_total = jnp.zeros(signal.shape, jnp.float32)
    end_list = []
    for mode_index in range(residues.shape[0]):
        rate_mode = mode_rates[mode_index]
        weight = residues[mode_index] * jnp.sqrt(rate_mode)
        rising = jnp.exp(rate_mode * centred)
        falling = jnp.exp(-rate_mode * centred)
        running = falling * jnp.dot(lower, rising * signal, precision=precise)
        local_total = local_total + weight * running
        end_list.append(running[tok_rows - 1])
    end_states = jnp.stack(end_list)
    block_decay = jnp.exp(-mode_rates * tok_rows)
    identity = (jnp.zeros(end_states.shape, jnp.float32), jnp.ones(end_states.shape, jnp.float32))
    carried, _ = carried_in((end_states, block_decay), "seq", carry_states, identity)
    after = (steps.astype(jnp.float32) + 1.0)[:, None]
    for mode_index in range(residues.shape[0]):
        rate_mode = mode_rates[mode_index]
        weight = residues[mode_index] * jnp.sqrt(rate_mode)
        local_total = local_total + weight * carried[mode_index] * jnp.exp(-rate_mode * after)
    rounded = lax.optimization_barrier(local_total.astype(jnp.bfloat16))
    return rounded.astype(jnp.float32)


def per_device(
    tokens, query_in, key_in, proj_in, proj_out, short_taps, residues, mode_rates, skip_gain
):
    tok_rows = tokens.shape[0]
    margin_rows = short_taps.shape[1] - 1
    partial_value = jnp.dot(
        tokens,
        lax.all_gather(proj_in, "seq", axis=1, tiled=True),
        preferred_element_type=jnp.float32,
    )
    low_rank = lax.psum(partial_value, "ch").astype(jnp.bfloat16)
    value_full = jnp.dot(
        low_rank,
        lax.all_gather(proj_out, "seq", axis=0, tiled=True),
        preferred_element_type=jnp.float32,
    )
    value_proj = value_full.astype(jnp.bfloat16)
    edges = jnp.stack(
        [
            query_in[tok_rows - margin_rows :],
            key_in[tok_rows - margin_rows :],
            value_proj[tok_rows - margin_rows :],
        ]
    )
    arrived_edges = passed_along(edges, "seq", 1)
    query_previous = arrived_edges[0]
    key_previous = arrived_edges[1]
    value_previous = arrived_edges[2]
    query_short = short_filter(query_previous, query_in, short_taps[0])
    key_short = short_filter(key_previous, key_in, short_taps[1])
    value_short = short_filter(value_previous, value_proj, short_taps[2])
    mixed = (key_short * value_short).astype(jnp.bfloat16)
    convolved_tokens = modal_convolve(mixed, residues, mode_rates)
    return (query_short * (convolved_tokens + skip_gain * mixed.astype(jnp.float32))).astype(
        jnp.bfloat16
    )


def chosen(mesh):
    def run(*args):
        rows, channels = args[0].shape
        ranks = args[3].shape[1]
        square = mesh.shape["seq"] == GROUP * GROUP and mesh.shape["ch"] == 2
        whole = channels % (GROUP * 1024) == 0 and ranks % 32 == 0 and rows % 32 == 0
        fits = (GROUP * ranks) % 128 == 0 and channels == GROUP * 1024
        fits = fits and args[5].shape[1] <= 16
        return (planes_device if square and whole and fits else per_device)(*args)

    return run


def solution(mesh):
    placed = (
        P("seq", "ch"),
        P("seq", "ch"),
        P("seq", "ch"),
        P("ch", "seq"),
        P("seq", "ch"),
        P(None, None, "ch"),
        P(None, "ch"),
        P(None, "ch"),
        P("ch"),
    )
    return jax.shard_map(
        chosen(mesh), mesh=mesh, in_specs=placed, out_specs=P("seq", "ch"), check_vma=False
    )
```

```python
import functools

import jax
import jax.numpy as jnp
from jax import lax
from jax.experimental import pallas as pl
from jax.experimental.pallas import tpu as pltpu
from jax.sharding import PartitionSpec as P

MESH = pl.DeviceIdType.MESH
VMEM = pl.BlockSpec(memory_space=pltpu.VMEM)
ANY = pl.BlockSpec(memory_space=pl.ANY)
GROUP = 4


def where_am_i():
    me = lax.axis_index("seq")
    return me // GROUP, me % GROUP


def device(plane, spot):
    return {"seq": plane * GROUP + spot}


def remote(source, target, sems, index, place):
    return pltpu.make_async_remote_copy(
        src_ref=source, dst_ref=target, send_sem=sems[0].at[index], recv_sem=sems[1].at[index],
        device_id=place, device_id_type=MESH,
    )


def greet(places):
    barrier = pltpu.get_barrier_semaphore()
    for place in places:
        pl.semaphore_signal(barrier, inc=1, device_id=place, device_id_type=MESH)
    pl.semaphore_wait(barrier, len(places))


def multiple(value, by):
    return pl.multiple_of(value, by)


class Place:
    def __init__(self):
        self.me, self.core = lax.axis_index("seq"), lax.axis_index("ch")
        self.count = lax.axis_size("seq")
        self.plane, self.spot = self.me // GROUP, self.me % GROUP
        plane, spot = self.plane, self.spot
        self.side = plane // 2
        self.outer = (self.side + plane + 1) % 2
        self.mate, self.cross = plane + 1 - 2 * (plane % 2), 3 - plane
        self.far = 3 - self.mate
        self.peers = [spot, spot + 1 - 2 * (spot % 2), (spot + 2) % GROUP, 3 - spot]
        self.partner = {"ch": 1 - self.core}

    def at_outer(self, run):
        pl.when(self.outer == 1)(run)

    def at_inner(self, run):
        pl.when(self.outer == 0)(run)


CUTS = 4
AGAIN = range(1, GROUP)
W1A, W2A, TOK, KEY = 0, 3, 6, 9
W1M, W1C, TOKM = 12, 16, 24
W2M, W2C, W2CM, W2O, W2F = 28, 32, 36, 40, 44
PAIR, RS, LZ, AG, LD = 48, 56, 72, 74, 80
EDGE, QT, KT, KM = 88, 89, 90, 91
COPIES = 94


def fetch_all(
    tok, pin, pout, key, query, low_out, rows_out, key_out, query_edge,
    w1, tok_all, w2, key_all, key_edge, partial, inbox, summed, parts, mylow, lowout, low_all,
    send, recv, local,
):
    p = Place()
    plane, spot, core, peers = p.plane, p.spot, p.core, p.peers
    rows, ranks, width = tok.shape[0], pin.shape[0], w2.shape[-1]
    margin, half = query_edge.shape[0], rows // 2
    share, both = GROUP * ranks, GROUP * GROUP * ranks
    wide, sub = both // 2, width // CUTS
    after = {"seq": (p.me + 1) % p.count}
    before = {"seq": (p.me + p.count - 1) % p.count}

    barrier = pltpu.get_barrier_semaphore()
    greeted = [device(plane, peers[k]) for k in AGAIN]
    greeted += [device(p.mate, spot), p.partner, after, before]
    for place in greeted:
        pl.semaphore_signal(barrier, inc=1, device_id=place, device_id_type=MESH)

    @p.at_inner
    def _():
        pl.semaphore_signal(barrier, inc=1, device_id=device(p.cross, spot), device_id_type=MESH)

    pl.semaphore_wait(barrier, len(greeted) + 1 - p.outer)

    def go(source, target, index, place):
        return remote(source, target, (send, recv), index, place)

    def cols(s):
        return pl.ds(multiple(s * width, width), width)

    def w1_rows(at, s):
        return pl.ds(multiple((at * GROUP + s) * ranks, ranks), ranks)

    def tok_rows(b, s):
        return pl.ds(multiple((b * GROUP + s) * rows, rows), rows)

    def cut(c):
        return slice(c * sub, (c + 1) * sub)

    def halves(h):
        return pl.ds(multiple(h * wide, wide), wide)

    def low_rows(s, j):
        return pl.ds(multiple(margin + s * rows + j * half, margin), half)

    def scatter(source, target, base):
        return [go(source(peers[k]), target, base + k - 1, device(plane, peers[k])) for k in AGAIN]

    mate_dev, cross_dev = device(p.mate, spot), device(p.cross, spot)
    mine1 = w1.at[w1_rows(plane, spot)]
    w1_swap = scatter(lambda s: pin.at[:, cols(s)], mine1, W1A)
    tok_swap = scatter(lambda s: tok.at[:, cols(s)], tok_all.at[tok_rows(p.outer, spot)], TOK)
    w2_swap = scatter(lambda s: pout.at[:, cols(s)], w2.at[plane, spot], W2A)
    key_rows = pl.ds(multiple(margin + spot * rows, margin), rows)
    key_swap = scatter(lambda s: key.at[:, cols(s)], key_all.at[key_rows], KEY)
    tails = [
        go(key.at[pl.ds(rows - margin, margin)], key_edge, KT, after),
        go(query.at[pl.ds(rows - margin, margin)], query_edge, QT, after),
    ]

    def key_margin(k):
        return go(key_edge.at[:, cols(peers[k])], key_all.at[pl.ds(0, margin)], KM + k - 1,
                  device(plane, peers[k]))

    def start_tails():
        run(tails, "start")

    def share_tails():
        @pl.when(p.me > 0)
        def _():
            run(tails, "wait_recv")

        @pl.when((spot == 0) & (plane > 0))
        def _():
            for k in AGAIN:
                key_margin(k).start()
            key_all[0:margin, :] = key_edge[:, cols(spot)]

        run(key_swap, "start")

        @pl.when(plane == 0)
        def _():
            key_all[0:margin, :] = jnp.zeros((margin, width), key_all.dtype)

    def end_tails():
        run(key_swap, "wait_recv")
        for k in AGAIN:
            pl.when((spot == k) & (plane > 0))(key_margin(k).wait_recv)

        @pl.when((spot == 0) & (plane > 0))
        def _():
            for k in AGAIN:
                key_margin(k).wait_send()

        @pl.when(p.me < p.count - 1)
        def _():
            run(tails, "wait_send")

    def own_or(first, arrived, k):
        return first if k == 0 else arrived

    w1_mate = [
        go(own_or(pin.at[:, cols(spot)], w1.at[w1_rows(plane, peers[k])], k),
           w1.at[w1_rows(plane, peers[k])], W1M + k, mate_dev) for k in range(GROUP)]
    w1_cross = [
        go(own_or(pin.at[:, cols(spot)], w1.at[w1_rows(plane, peers[k])], k),
           w1.at[w1_rows(plane, peers[k])], W1C + k, cross_dev) for k in range(GROUP)]
    w1_on = [
        go(w1.at[w1_rows(p.mate, peers[k])], w1.at[w1_rows(p.mate, peers[k])],
           W1C + GROUP + k, cross_dev) for k in range(GROUP)]
    tok_mate = [
        go(own_or(tok.at[:, cols(spot)], tok_all.at[tok_rows(1, peers[k])], k),
           tok_all.at[tok_rows(1, peers[k])], TOKM + k, mate_dev) for k in range(GROUP)]

    def strip(at, c, base, place):
        block = w2.at[at, :, :, cut(c)]
        return go(block, block, base + c, place)

    every = range(CUTS)
    w2_mate = [strip(plane, c, W2M, mate_dev) for c in every]
    w2_cross = [strip(plane, c, W2C, cross_dev) for c in every]
    w2_on = [strip(p.mate, c, W2CM, cross_dev) for c in every]
    w2_out = [strip(p.cross, c, W2O, mate_dev) for c in every]
    w2_far = [strip(p.far, c, W2F, mate_dev) for c in every]

    def run(copies, what):
        for copy in copies:
            getattr(copy, what)()

    run(w1_swap, "start")
    p.at_outer(w1_mate[0].start)
    p.at_outer(tok_mate[0].start)
    p.at_inner(w1_cross[0].start)
    run(tok_swap, "start")
    run(w2_swap, "start")
    pl.when(p.me < p.count - 1)(start_tails)
    w1[w1_rows(plane, spot), :] = pin[:, cols(spot)]
    tok_all[tok_rows(p.outer, spot), :] = tok[:, cols(spot)]
    keep = [
        pltpu.make_async_copy(pout.at[:, cols(spot)], w2.at[plane, spot], local.at[0]),
        pltpu.make_async_copy(key.at[:, cols(spot)], key_all.at[key_rows], local.at[1]),
    ]
    run(keep, "start")
    run(keep, "wait")

    order = [plane, p.cross, p.mate, p.far]

    def quarter(q):
        return pl.ds(multiple(order[q] * share, share), share)

    def multiply(left, place):
        return lax.dot_general(
            left, w1[place, :], (((1,), (1,)), ((), ())), preferred_element_type=jnp.float32)

    def pair(u):
        if u < GROUP:
            source = partial.at[0, :, 1 - core, :, quarter(u)]
            target = inbox.at[0, :, :, quarter(u)]
        else:
            spot_at = peers[u - GROUP]
            source, target = partial.at[1, spot_at, 1 - core], inbox.at[1, spot_at]
        return go(source, target, PAIR + u, p.partner)

    def unit(q):
        found = multiply(tok_all[0:GROUP * rows, :], quarter(q))
        partial[0, :, :, :, quarter(q)] = found.reshape(GROUP, 2, half, share)
        pair(q).start()

    def row_unit(k):
        left = tok_all[tok_rows(1, peers[k]), :]
        for n in range(both // 256):
            found = multiply(left, slice(n * 256, (n + 1) * 256))
            partial[1, peers[k], :, :, n * 256:(n + 1) * 256] = found.reshape(2, half, 256)
        pair(GROUP + k).start()

    def reduced(q):
        return [
            go(summed.at[0, peers[k], :, quarter(q)], parts.at[k - 1, 0, :, quarter(q)],
               RS + 3 * q + k - 1, device(plane, peers[k])) for k in AGAIN]

    def row_reduced(k):
        return go(summed.at[1, peers[k]], parts.at[k - 1, 1], RS + 11 + k, device(plane, peers[k]))

    def add_pair(q):
        pair(q).wait_recv()
        place = quarter(q)
        for s in range(GROUP):
            summed[0, s, :, place] = (
                partial[0, s, core, :, place] + inbox[0, s, :, place]).astype(summed.dtype)
        run(reduced(q), "start")

    def row_add(k):
        pair(GROUP + k).wait_recv()
        if k:
            at = peers[k]
            summed[1, at] = (partial[1, at, core] + inbox[1, at]).astype(summed.dtype)
            row_reduced(k).start()

    def finish(b):
        if b:
            run([row_reduced(k) for k in AGAIN], "wait_recv")
        else:
            for q in range(GROUP):
                run(reduced(q), "wait_recv")
        total = partial[b, spot, core] + inbox[b, spot]
        for k in AGAIN:
            total = total + parts[k - 1, b].astype(jnp.float32)
        target = lowout if b else mylow
        target[...] = total.astype(target.dtype)

    def low_up(h):
        return go(lowout.at[:, halves(h)], mylow.at[:, halves(h)], LZ + h, mate_dev)

    def gather(h):
        return [
            go(mylow.at[:, halves(h)], low_all.at[low_rows(spot, core), halves(h)],
               AG + 3 * h + k - 1, device(plane, peers[k])) for k in AGAIN]

    def across(h, k):
        block = low_all.at[low_rows(peers[k], core), halves(h)]
        return go(own_or(mylow.at[:, halves(h)], block, k), block, LD + 4 * h + k, p.partner)

    def spread_low(h):
        run(gather(h), "start")
        across(h, 0).start()
        low_all[low_rows(spot, core), halves(h)] = mylow[:, halves(h)]

    @p.at_outer
    def _():
        for k in (1, 2):
            w1_swap[k - 1].wait_recv()
            w1_mate[k].start()
        tok_swap[0].wait_recv()
        tok_mate[1].start()
        w1_swap[2].wait_recv()
        w1_mate[3].start()
        for k in (2, 3):
            tok_swap[k - 1].wait_recv()
            tok_mate[k].start()
        run(w2_swap, "wait_recv")
        run(w2_mate, "start")
        share_tails()

    @p.at_inner
    def _():
        def forward(copies, on, which):
            for k in which:
                copies[k].wait_recv()
                on[k].start()

        for k in (1, 2):
            w1_swap[k - 1].wait_recv()
            w1_cross[k].start()
        forward(w1_mate, w1_on, (0,))
        w1_swap[2].wait_recv()
        w1_cross[3].start()
        forward(w1_mate, w1_on, (1, 2))
        run(tok_swap, "wait_recv")
        unit(0)
        run(w1_cross, "wait_recv")
        unit(1)
        add_pair(0)
        add_pair(1)
        forward(w1_mate, w1_on, (3,))
        unit(2)
        run(w2_swap, "wait_recv")
        run(w2_cross, "start")
        run(w2_mate, "start")
        add_pair(2)
        run(w1_on, "wait_recv")
        unit(3)
        tok_mate[0].wait_recv()
        row_unit(0)
        add_pair(3)
        tok_mate[1].wait_recv()
        row_unit(1)
        row_add(0)
        tok_mate[2].wait_recv()
        row_unit(2)
        row_add(1)
        tok_mate[3].wait_recv()
        row_unit(3)
        row_add(2)
        row_add(3)
        forward(w2_cross, w2_out, (0,))
        finish(0)
        for h in range(2):
            spread_low(h)
        forward(w2_cross, w2_out, (1,))
        forward(w2_mate, w2_on, (0,))
        finish(1)
        for h in range(2):
            low_up(h).start()
        share_tails()
        forward(w2_cross, w2_out, (2,))
        forward(w2_mate, w2_on, (1,))
        forward(w2_cross, w2_out, (3,))
        forward(w2_mate, w2_on, (2, 3))

    @p.at_outer
    def _():
        for h in (0, 1):
            low_up(h).wait_recv()
            spread_low(h)

    for h in (0, 1):
        for k in AGAIN:
            gather(h)[k - 1].wait_recv()
            across(h, k).start()

    @p.at_inner
    def _():
        for c in every:
            w2_on[c].wait_recv()
            w2_far[c].start()

    for h in (0, 1):
        for k in range(GROUP):
            across(h, k).wait_recv()
    above = go(low_all.at[pl.ds(low_all.shape[0] - margin, margin)],
               low_all.at[pl.ds(0, margin)], EDGE, device((plane + 1) % GROUP, spot))
    pl.when(plane < GROUP - 1)(above.start)

    @p.at_outer
    def _():
        run(w2_mate + w2_out + w2_far, "wait_recv")

    pl.when(plane > 0)(above.wait_recv)

    @pl.when(plane == 0)
    def _():
        low_all[0:margin, :] = jnp.zeros((margin, both), low_all.dtype)

    end_tails()
    out = [
        pltpu.make_async_copy(key_all, key_out, local.at[2]),
        pltpu.make_async_copy(low_all, low_out, local.at[3]),
        pltpu.make_async_copy(w2, rows_out, local.at[4]),
    ]
    run(out, "start")
    run(w1_swap + w2_swap + tok_swap + key_swap, "wait_send")
    for h in (0, 1):
        run(gather(h) + [across(h, k) for k in range(GROUP)], "wait_send")
    pl.when(plane < GROUP - 1)(above.wait_send)
    run(w2_mate, "wait_send")

    @p.at_outer
    def _():
        run(w1_mate + tok_mate, "wait_send")

    @p.at_inner
    def _():
        run(w1_cross + w1_on + w2_cross + w2_on + w2_out + w2_far, "wait_send")
        for u in range(2 * GROUP):
            pair(u).wait_send()
        for u in range(GROUP):
            run(reduced(u), "wait_send")
        for k in AGAIN:
            row_reduced(k).wait_send()
        for h in range(2):
            low_up(h).wait_send()

    run(out, "wait")


SEGMENTS = 8
LANES = 128
ENDS, GIVE = 0, 24
TAIL_COPIES = 36


def one_hot(rows, columns, target):
    row = lax.broadcasted_iota(jnp.int32, (rows, columns), 0)
    column = lax.broadcasted_iota(jnp.int32, (rows, columns), 1)
    return (column == target(row)).astype(jnp.bfloat16)


def convolve(
    low_all, w2, key_all, query, query_edge, taps, residues, rates, skip, out,
    low_mixed, keys, values, mixed, kept, turned, given, gains, decay, weight, direct, longer,
    states, mine, ends, send, recv,
):
    p = Place()
    plane, spot, peers = p.plane, p.spot, p.peers
    f32, bf16 = jnp.float32, jnp.bfloat16
    margin, rows = query_edge.shape[0], query.shape[0]
    modes, width = decay.shape[0], values.shape[1]
    count = taps.shape[1]
    all_rows = rows * GROUP
    steps = all_rows // SEGMENTS
    lead = SEGMENTS
    spread_rows = (steps + lead) * SEGMENTS
    strip = width // CUTS
    tiles = width // LANES
    both = low_all.shape[1]

    barrier = pltpu.get_barrier_semaphore()
    greeted = [device(plane, peers[k]) for k in AGAIN]
    greeted += [device((plane + d) % GROUP, spot) for d in AGAIN]
    for place in greeted:
        pl.semaphore_signal(barrier, inc=1, device_id=place, device_id_type=MESH)
    pl.semaphore_wait(barrier, len(greeted))

    def go(source, target, index, place):
        return remote(source, target, (send, recv), index, place)

    spread = one_hot(
        spread_rows, margin + all_rows,
        lambda row: margin - lead + steps * (row % SEGMENTS) + row // SEGMENTS)
    gather = one_hot(
        all_rows, all_rows, lambda row: SEGMENTS * (row % steps) + row // steps)

    def dot(left, right):
        return jnp.dot(left, right, preferred_element_type=f32)

    for n in range(both // 256):
        at = slice(n * 256, (n + 1) * 256)
        low_mixed[:, at] = dot(spread, low_all[:, at]).astype(bf16)
    for c in range(CUTS):
        at = slice(c * strip, (c + 1) * strip)
        keys[:, at] = dot(spread, key_all[:, at])
    own = pl.ds(multiple(spot * width, width), width)

    def rows_of(vector):
        return jnp.broadcast_to(vector, (SEGMENTS, width))

    for branch in range(2):
        for tap in range(count):
            gains[branch, tap] = rows_of(taps[branch + 1, pl.ds(tap, 1), own])
    for mode in range(modes):
        rate = rows_of(rates[pl.ds(mode, 1), own])
        decay[mode] = jnp.exp(-rate)
        longer[mode] = rate
        weight[mode] = rows_of(residues[pl.ds(mode, 1), own]) * jnp.sqrt(rate)
    direct[...] = rows_of(skip[pl.ds(0, 1), own])

    for c in range(CUTS):
        at = slice(c * strip, (c + 1) * strip)
        found = dot(low_mixed[...], w2[:, :, :, at].reshape(both, strip))
        values[:, at] = found.astype(bf16).astype(f32)

    def lane(tile):
        return pl.ds(multiple(tile * LANES, LANES), LANES)

    def at_step(j):
        return pl.ds(multiple(j * SEGMENTS, SEGMENTS), SEGMENTS)

    sub = lax.broadcasted_iota(jnp.int32, (SEGMENTS, LANES), 0)

    def down(value, by):
        return jnp.where(sub >= by, pltpu.roll(value, by, 0), 0.0)

    def mix(tile):
        cols = lane(tile)
        tap = [[gains[b, t, :, cols] for t in range(count)] for b in range(2)]

        def filtered(source, b, j):
            total = None
            for t in range(count):
                term = tap[b][t] * source[at_step(j + lead - t), cols]
                total = term if total is None else total + term
            return total

        @pl.loop(0, steps // 8)
        def _(block):
            for part in range(8):
                j = block * 8 + part
                product = filtered(keys, 0, j) * filtered(values, 1, j)
                mixed[at_step(j), cols] = product.astype(bf16).astype(f32)

    def end_of(tile):
        cols = lane(tile)
        factor = [decay[n, :, cols] for n in range(modes)]

        def body(block, held):
            for part in range(8):
                value = mixed[at_step(block * 8 + part), cols]
                held = [h * r + value for h, r in zip(held, factor)]
            return held

        held = lax.fori_loop(0, steps // 8, body, [jnp.zeros((SEGMENTS, LANES), f32)] * modes)
        for n in range(modes):
            rate = longer[n, :, cols]
            total = held[n]
            for power in (1, 2, 4):
                total = total + jnp.exp(-rate * (steps * power)) * down(total, power)
            states[n, :, cols] = down(total, 1)
            mine[tile, pl.ds(n, 1), :] = total[SEGMENTS - 1:, :]

    def ends_copy(tile, d):
        return go(mine.at[tile], ends.at[tile, d - 1], ENDS + tile * 3 + d - 1,
                  device((plane + d) % GROUP, spot))

    def share(tile):
        for d in AGAIN:
            pl.when(plane + d < GROUP)(ends_copy(tile, d).start)

    def arrive(tile):
        for d in AGAIN:
            pl.when(plane >= d)(ends_copy(tile, d).wait_recv)

    def conv(tile):
        cols = lane(tile)
        factor = [decay[n, :, cols] for n in range(modes)]
        start = []
        for n in range(modes):
            rate = longer[n, :, cols]
            row = rate[0:1]
            total = jnp.zeros((1, LANES), f32)
            for d in reversed(AGAIN):
                far = jnp.exp(-row * (all_rows * (d - 1))) * ends[tile, d - 1, pl.ds(n, 1), :]
                total = jnp.where(plane >= d, total + far, total)
            spent = jnp.exp(-rate * (steps * sub.astype(f32)))
            start.append(states[n, :, cols] + spent * total)
        gain = direct[:, cols]

        def body(block, held):
            pair = []
            for part in range(4):
                value = mixed[at_step(block * 4 + part), cols]
                held = [h * r + value for h, r in zip(held, factor)]
                terms = [h * weight[n, :, cols] for n, h in enumerate(held)]
                while len(terms) > 1:
                    terms = [a + b for a, b in zip(terms[::2], terms[1::2])]
                pair.append(terms[0].astype(bf16).astype(f32) + gain * value)
            place = pl.ds(multiple(block * 4 * SEGMENTS, 4 * SEGMENTS), 4 * SEGMENTS)
            kept[place, cols] = jnp.concatenate(pair, axis=0).astype(bf16)
            return held

        lax.fori_loop(0, steps // 4, body, start)

    def give(c, k):
        at = slice(c * strip, (c + 1) * strip)
        here = pl.ds(multiple(peers[k] * rows, rows), rows)
        there = pl.ds(multiple(spot * width + c * strip, strip), strip)
        return go(turned.at[here, at], given.at[:, there], GIVE + 3 * c + k - 1,
                  device(plane, peers[k]))

    def turn(c):
        at = slice(c * strip, (c + 1) * strip)
        turned[:, at] = dot(gather, kept[:, at]).astype(bf16)
        for k in AGAIN:
            give(c, k).start()

    on = p.me > 0

    def product(s, c, block):
        cols = pl.ds(multiple(s * width + c * strip, strip), strip)
        edge = jnp.where(on, query_edge[:, cols].astype(f32), 0.0)
        signal = jnp.concatenate([edge, query[:, cols].astype(f32)], axis=0)
        total = None
        for t in range(count):
            term = taps[0, pl.ds(t, 1), cols] * signal[margin - t:margin - t + rows]
            total = term if total is None else total + term
        out[:, cols] = (total * block.astype(f32)).astype(out.dtype)

    @pl.loop(0, tiles)
    def _(tile):
        mix(tile)
        end_of(tile)
        share(tile)

    for c in range(CUTS):

        @pl.loop(c * (tiles // CUTS), (c + 1) * (tiles // CUTS))
        def _(tile):
            arrive(tile)
            conv(tile)

        turn(c)

    for c in range(CUTS):
        mine_rows = pl.ds(multiple(spot * rows, rows), rows)
        product(spot, c, turned[mine_rows, c * strip:(c + 1) * strip])
    for c in range(CUTS):
        for k in AGAIN:
            give(c, k).wait_recv()
            at = pl.ds(multiple(peers[k] * width + c * strip, strip), strip)
            product(peers[k], c, given[:, at])
    for c in range(CUTS):
        for k in AGAIN:
            give(c, k).wait_send()

    @pl.loop(0, tiles)
    def _(tile):
        for d in AGAIN:
            pl.when(plane + d < GROUP)(ends_copy(tile, d).wait_send)


def talk(kernel, shapes, in_specs, scratch, copies, locals_, ident):
    one = not isinstance(shapes, (list, tuple))
    return pl.pallas_call(
        kernel,
        out_shape=shapes,
        in_specs=in_specs,
        out_specs=ANY if one else [ANY] * len(shapes),
        scratch_shapes=scratch + [
            pltpu.SemaphoreType.DMA((copies,)),
            pltpu.SemaphoreType.DMA((copies,)),
            pltpu.SemaphoreType.DMA((locals_,)),
        ],
        compiler_params=pltpu.CompilerParams(collective_id=ident, has_side_effects=True),
    )


def planes_device(
    tokens, query_in, key_in, proj_in, proj_out, short_taps, residues, mode_rates, skip_gain
):
    rows, channels = tokens.shape
    ranks = proj_in.shape[1]
    modes = residues.shape[0]
    margin_rows = short_taps.shape[1] - 1
    width, all_rows = channels // GROUP, rows * GROUP
    tall = width // 128
    half = jnp.bfloat16
    shape = jax.ShapeDtypeStruct
    plane, spot = where_am_i()
    margin = 16
    share, both = GROUP * ranks, GROUP * GROUP * ranks

    full, band = jnp.float32, rows // 2
    low_all, rows_all, key_all, query_edge = talk(
        fetch_all,
        [shape((margin + all_rows, both), half), shape((GROUP, GROUP, ranks, width), half),
         shape((margin + all_rows, width), half), shape((margin, channels), half)],
        [VMEM] * 5,
        [pltpu.VMEM((both, width), half), pltpu.VMEM((2 * all_rows, width), half),
         pltpu.VMEM((GROUP, GROUP, ranks, width), half), pltpu.VMEM((margin + all_rows, width), half), pltpu.VMEM((margin, channels), half),
         pltpu.VMEM((2, GROUP, 2, band, both), full), pltpu.VMEM((2, GROUP, band, both), full),
         pltpu.VMEM((2, GROUP, band, both), half), pltpu.VMEM((GROUP - 1, 2, band, both), half),
         pltpu.VMEM((band, both), half), pltpu.VMEM((band, both), half),
         pltpu.VMEM((margin + all_rows, both), half)],
        COPIES, 7, 5,
    )(tokens, proj_in.T, proj_out, key_in, query_in)
    spread_rows = all_rows + SEGMENTS * SEGMENTS
    eight = pltpu.VMEM((modes, SEGMENTS, width), full)
    return pl.pallas_call(
        convolve,
        out_shape=shape((rows, channels), half),
        in_specs=[VMEM] * 9, out_specs=VMEM,
        scratch_shapes=[
            pltpu.VMEM((spread_rows, both), half), pltpu.VMEM((spread_rows, width), full),
            pltpu.VMEM((spread_rows, width), full), pltpu.VMEM((all_rows, width), full),
            pltpu.VMEM((all_rows, width), half), pltpu.VMEM((all_rows, width), half),
            pltpu.VMEM((rows, channels), half),
            pltpu.VMEM((2, margin_rows + 1, SEGMENTS, width), full), eight, eight,
            pltpu.VMEM((SEGMENTS, width), full), eight, eight,
            pltpu.VMEM((width // LANES, modes, LANES), full),
            pltpu.VMEM((width // LANES, GROUP - 1, modes, LANES), full),
            pltpu.SemaphoreType.DMA((TAIL_COPIES,)), pltpu.SemaphoreType.DMA((TAIL_COPIES,))],
        compiler_params=pltpu.CompilerParams(collective_id=2, has_side_effects=True),
    )(low_all, rows_all, key_all, query_in, query_edge, short_taps, residues, mode_rates,
      skip_gain[None])


precise = lax.Precision.HIGHEST


def carried_in(value, axis, join, neutral):
    count, mine = (lax.axis_size(axis), lax.axis_index(axis))
    pieces = jax.tree.map(lambda part: lax.all_gather(part, axis), value)
    total = jax.tree.map(
        lambda part, zero: jnp.full_like(part, 0) + jnp.asarray(zero, part.dtype), value, neutral
    )

    def turn(position, total):
        longer = join(total, jax.tree.map(lambda part: part[position], pieces))
        return jax.tree.map(lambda new, old: jnp.where(position < mine, new, old), longer, total)

    return lax.fori_loop(0, count - 1, turn, total)


def passed_along(value, axis, steps):
    count = lax.axis_size(axis)
    leading, last = (max(0, -steps), min(count, count - steps))
    return lax.ppermute(value, axis, [(source, source + steps) for source in range(leading, last)])


def short_filter(previous, current, filter_taps):
    margin_rows = filter_taps.shape[0] - 1
    length = current.shape[0]
    extended = jnp.concatenate([previous, current], axis=0).astype(jnp.float32)
    result = filter_taps[0] * extended[margin_rows : margin_rows + length]
    for offset in range(1, margin_rows + 1):
        result = (
            result
            + filter_taps[offset] * extended[margin_rows - offset : margin_rows - offset + length]
        )
    return result


def carry_states(earlier, later):
    return (earlier[0] * later[1] + later[0], earlier[1] * later[1])


def modal_convolve(mixed, residues, mode_rates):
    tok_rows = mixed.shape[0]
    signal = mixed.astype(jnp.float32)
    steps = jnp.arange(tok_rows, dtype=jnp.int32)
    lower = (steps[:, None] >= steps[None, :]).astype(jnp.float32)
    centred = (steps.astype(jnp.float32) - 0.5 * tok_rows)[:, None]
    local_total = jnp.zeros(signal.shape, jnp.float32)
    end_list = []
    for mode_index in range(residues.shape[0]):
        rate_mode = mode_rates[mode_index]
        weight = residues[mode_index] * jnp.sqrt(rate_mode)
        rising = jnp.exp(rate_mode * centred)
        falling = jnp.exp(-rate_mode * centred)
        running = falling * jnp.dot(lower, rising * signal, precision=precise)
        local_total = local_total + weight * running
        end_list.append(running[tok_rows - 1])
    end_states = jnp.stack(end_list)
    block_decay = jnp.exp(-mode_rates * tok_rows)
    identity = (jnp.zeros(end_states.shape, jnp.float32), jnp.ones(end_states.shape, jnp.float32))
    carried, _ = carried_in((end_states, block_decay), "seq", carry_states, identity)
    after = (steps.astype(jnp.float32) + 1.0)[:, None]
    for mode_index in range(residues.shape[0]):
        rate_mode = mode_rates[mode_index]
        weight = residues[mode_index] * jnp.sqrt(rate_mode)
        local_total = local_total + weight * carried[mode_index] * jnp.exp(-rate_mode * after)
    rounded = lax.optimization_barrier(local_total.astype(jnp.bfloat16))
    return rounded.astype(jnp.float32)


def per_device(
    tokens, query_in, key_in, proj_in, proj_out, short_taps, residues, mode_rates, skip_gain
):
    tok_rows = tokens.shape[0]
    margin_rows = short_taps.shape[1] - 1
    partial_value = jnp.dot(
        tokens,
        lax.all_gather(proj_in, "seq", axis=1, tiled=True),
        preferred_element_type=jnp.float32,
    )
    low_rank = lax.psum(partial_value, "ch").astype(jnp.bfloat16)
    value_full = jnp.dot(
        low_rank,
        lax.all_gather(proj_out, "seq", axis=0, tiled=True),
        preferred_element_type=jnp.float32,
    )
    value_proj = value_full.astype(jnp.bfloat16)
    edges = jnp.stack(
        [
            query_in[tok_rows - margin_rows :],
            key_in[tok_rows - margin_rows :],
            value_proj[tok_rows - margin_rows :],
        ]
    )
    arrived_edges = passed_along(edges, "seq", 1)
    query_previous = arrived_edges[0]
    key_previous = arrived_edges[1]
    value_previous = arrived_edges[2]
    query_short = short_filter(query_previous, query_in, short_taps[0])
    key_short = short_filter(key_previous, key_in, short_taps[1])
    value_short = short_filter(value_previous, value_proj, short_taps[2])
    mixed = (key_short * value_short).astype(jnp.bfloat16)
    convolved_tokens = modal_convolve(mixed, residues, mode_rates)
    return (query_short * (convolved_tokens + skip_gain * mixed.astype(jnp.float32))).astype(
        jnp.bfloat16
    )


def chosen(mesh):
    def run(*args):
        rows, channels = args[0].shape
        ranks = args[3].shape[1]
        square = mesh.shape["seq"] == GROUP * GROUP and mesh.shape["ch"] == 2
        whole = channels % (GROUP * 1024) == 0 and ranks % 32 == 0 and rows % 32 == 0
        fits = (GROUP * ranks) % 128 == 0 and channels == GROUP * 1024
        fits = fits and args[5].shape[1] <= 16
        return (planes_device if square and whole and fits else per_device)(*args)

    return run


def solution(mesh):
    placed = (
        P("seq", "ch"),
        P("seq", "ch"),
        P("seq", "ch"),
        P("ch", "seq"),
        P("seq", "ch"),
        P(None, None, "ch"),
        P(None, "ch"),
        P(None, "ch"),
        P("ch"),
    )
    return jax.shard_map(
        chosen(mesh), mesh=mesh, in_specs=placed, out_specs=P("seq", "ch"), check_vma=False
    )
```
